32 devices in a mesh: dp: 1 (over z), ep: 32 (over y, x, core).
Axes of the slice: x: 4, y: 4, z: 1, core: 2. Of those that a mesh axis runs over, the one named last changes fastest.
The devices are a block of a 4x4x8 slice.
Arguments:
- tokens: bfloat16 [49152, 768], P(('dp', 'ep'))
- w_gate: float32 [768, 128], replicated
- first_ids: int32 [49152], P(('dp', 'ep'))
- second_ids: int32 [49152], P(('dp', 'ep'))
- keep_two: int32 [49152], P(('dp', 'ep'))
- w_in: bfloat16 [128, 768, 3072], P('ep')
- w_out: bfloat16 [128, 3072, 768], P('ep')
Outputs:
- output: bfloat16 [49152, 768], P(('dp', 'ep'))
All inputs are finite; a program needn't handle non-finite values.
Results may differ from the reference program's by a relative error of at most 0.00484227.
Values are sent between devices in bfloat16 or wider.
A program may use at most 768 MiB of HBM per device.

```python
import functools
import jax
import jax.numpy as jnp
from jax import lax

MODEL_DIM = 768
FF_DIM = 3072
NUM_EXPERTS = 128
GROUP_TOKENS = 1536
GROUPS = 32
CAPACITY = 24


def draw_routes(route_key, total_tokens):
    key_first, key_shift, key_keep, key_perm = jax.random.split(route_key, 4)
    first_ids = jax.random.randint(key_first, (total_tokens,), 0, NUM_EXPERTS, dtype=jnp.int32)
    cover_ids = jax.random.permutation(key_perm, NUM_EXPERTS).astype(jnp.int32)
    first_ids = first_ids.at[:NUM_EXPERTS].set(cover_ids)
    shift_ids = jax.random.randint(key_shift, (total_tokens,), 1, NUM_EXPERTS, dtype=jnp.int32)
    second_ids = (first_ids + shift_ids) % NUM_EXPERTS
    keep_two = jax.random.randint(key_keep, (total_tokens,), 0, 2, dtype=jnp.int32)
    return first_ids, second_ids, keep_two


def setup_inputs(seed: int = 0, part: int = 0) -> dict:
    root_key = jax.random.key(seed)
    part_key = jax.random.fold_in(root_key, part)
    key_x, key_route = jax.random.split(part_key)
    key_gate, key_in, key_out = jax.random.split(jax.random.key(seed + 1), 3)
    total_tokens = GROUPS * GROUP_TOKENS
    tokens = jax.random.normal(key_x, (total_tokens, MODEL_DIM), jnp.float32).astype(jnp.bfloat16)
    w_gate = jax.random.normal(key_gate, (MODEL_DIM, NUM_EXPERTS), jnp.float32) * MODEL_DIM ** -0.5
    w_in = (jax.random.normal(key_in, (NUM_EXPERTS, MODEL_DIM, FF_DIM), jnp.float32) * MODEL_DIM ** -0.5).astype(jnp.bfloat16)
    w_out = (jax.random.normal(key_out, (NUM_EXPERTS, FF_DIM, MODEL_DIM), jnp.float32) * (2.0 / FF_DIM) ** 0.5).astype(jnp.bfloat16)
    first_ids, second_ids, keep_two = draw_routes(key_route, total_tokens)
    return {"tokens": tokens, "w_gate": w_gate, "first_ids": first_ids, "second_ids": second_ids, "keep_two": keep_two, "w_in": w_in, "w_out": w_out}


def route_group(tokens, w_gate, first_ids, second_ids, keep_two, num_experts, capacity):
    logits = jnp.dot(tokens.astype(jnp.float32), w_gate)
    gate_probs = jax.nn.softmax(logits, axis=-1)
    expert_ids = jnp.arange(num_experts, dtype=jnp.int32)
    hot_first = (first_ids[:, None] == expert_ids[None, :]).astype(jnp.int32)
    hot_second = (second_ids[:, None] == expert_ids[None, :]).astype(jnp.int32)
    gate_one = jnp.sum(jnp.where(hot_first > 0, gate_probs, 0.0), axis=1)
    gate_two = jnp.sum(jnp.where(hot_second > 0, gate_probs, 0.0), axis=1)
    gate_sum = gate_one + gate_two
    pos_one = jnp.sum((jnp.cumsum(hot_first, axis=0) - hot_first) * hot_first, axis=1)
    first_count = jnp.sum(hot_first, axis=0)
    hot_kept = hot_second * keep_two[:, None]
    pos_two = jnp.sum((jnp.cumsum(hot_kept, axis=0) - hot_kept + first_count[None, :]) * hot_second, axis=1)
    kept_one = pos_one < capacity
    kept_two = jnp.logical_and(pos_two < capacity, keep_two > 0)
    drop_slot = num_experts * capacity
    slot_one = jnp.where(kept_one, first_ids * capacity + pos_one, drop_slot)
    slot_two = jnp.where(kept_two, second_ids * capacity + pos_two, drop_slot)
    wt_one = jnp.where(kept_one, gate_one / gate_sum, 0.0)
    wt_two = jnp.where(kept_two, gate_two / gate_sum, 0.0)
    return slot_one, slot_two, wt_one, wt_two


def dispatch_group(tokens, slot_one, slot_two, num_slots):
    seq_len = tokens.shape[0]
    token_pos = jnp.arange(seq_len, dtype=jnp.int32)
    source = jnp.full((num_slots + 1,), seq_len, dtype=jnp.int32)
    source = source.at[slot_one].set(token_pos).at[slot_two].set(token_pos)
    return jnp.take(tokens, source[:num_slots], axis=0, mode="fill", fill_value=0)


def combine_group(expert_rows, slot_one, slot_two, wt_one, wt_two):
    row_one = jnp.take(expert_rows, slot_one, axis=0, mode="fill", fill_value=0).astype(jnp.float32)
    row_two = jnp.take(expert_rows, slot_two, axis=0, mode="fill", fill_value=0).astype(jnp.float32)
    return (wt_one[:, None] * row_one + wt_two[:, None] * row_two).astype(jnp.bfloat16)


def expert_step(operands):
    expert_in, up_weight, down_weight = operands
    hidden = jnp.maximum(jnp.dot(expert_in, up_weight, preferred_element_type=jnp.float32), 0.0).astype(jnp.bfloat16)
    return jnp.dot(hidden, down_weight, preferred_element_type=jnp.float32).astype(jnp.bfloat16)


def reference(tokens, w_gate, first_ids, second_ids, keep_two, w_in, w_out):
    num_slots = NUM_EXPERTS * CAPACITY
    groups = tokens.reshape(GROUPS, GROUP_TOKENS, MODEL_DIM)
    route = functools.partial(route_group, num_experts=NUM_EXPERTS, capacity=CAPACITY)
    slot_one, slot_two, wt_one, wt_two = jax.vmap(route, in_axes=(0, None, 0, 0, 0))(
        groups, w_gate, first_ids.reshape(GROUPS, GROUP_TOKENS), second_ids.reshape(GROUPS, GROUP_TOKENS), keep_two.reshape(GROUPS, GROUP_TOKENS))
    buffers = jax.vmap(functools.partial(dispatch_group, num_slots=num_slots))(groups, slot_one, slot_two)
    by_expert = buffers.reshape(GROUPS, NUM_EXPERTS, CAPACITY, MODEL_DIM).transpose(1, 0, 2, 3).reshape(NUM_EXPERTS, GROUPS * CAPACITY, MODEL_DIM)
    expert_out = lax.map(expert_step, (by_expert, w_in, w_out))
    expert_rows = expert_out.reshape(NUM_EXPERTS, GROUPS, CAPACITY, MODEL_DIM).transpose(1, 0, 2, 3).reshape(GROUPS, num_slots, MODEL_DIM)
    mixed = jax.vmap(combine_group)(expert_rows, slot_one, slot_two, wt_one, wt_two)
    return mixed.reshape(GROUPS * GROUP_TOKENS, MODEL_DIM)
```

```python
import functools
import jax
import jax.numpy as jnp
from jax import lax
from jax.experimental import pallas as pl
from jax.experimental.pallas import tpu as pltpu
from jax.sharding import PartitionSpec as P

F32, BF16, I32 = jnp.float32, jnp.bfloat16, jnp.int32
VMEM_LIMIT = 67_000_000


def iota(shape, axis):
    return lax.broadcasted_iota(I32, shape, axis)


def slots_by_row(first, second, keep, num_experts, local_experts, capacity):
    seq_len = first.shape[1]
    block = 256
    expert = iota((num_experts, seq_len), 0)
    hot_first = (expert == first).astype(F32)
    hot_second = (expert == second).astype(F32)
    hot_kept = hot_second * keep.astype(F32)
    hot = jnp.concatenate([hot_first, hot_kept], axis=0)
    before = (iota((block, block), 0) < iota((block, block), 1)).astype(BF16)
    count = jnp.zeros((2 * num_experts, 1), F32)
    earlier = []
    for start in range(0, seq_len, block):
        part = hot[:, start : start + block]
        earlier.append(jnp.dot(part.astype(BF16), before, preferred_element_type=F32) + count)
        count = count + jnp.sum(part, axis=1, keepdims=True)
    earlier = jnp.concatenate(earlier, axis=1)
    pos_one = jnp.sum(earlier[:num_experts] * hot_first, axis=0, keepdims=True)
    pos_two = jnp.sum((earlier[num_experts:] + count[:num_experts]) * hot_second, axis=0, keepdims=True)
    pos_one, pos_two = pos_one.astype(I32), pos_two.astype(I32)
    span = num_experts // local_experts * capacity

    def slot(ids, pos, kept):
        return jnp.where(kept, (ids % local_experts) * span + (ids // local_experts) * capacity + pos, -1)

    kept_two = jnp.logical_and(pos_two < capacity, keep > 0)
    return slot(first, pos_one, pos_one < capacity), slot(second, pos_two, kept_two)


def columns_of(rows, seq_len):
    sublane = iota((128, seq_len), 0)
    stacked = jnp.zeros((128, seq_len), F32)
    for i, row in enumerate(rows):
        stacked = jnp.where(sublane == i, row.astype(F32), stacked)
    return stacked.T


def gates_of(tokens, w_gate, first, second):
    num_experts = w_gate.shape[1]
    high = w_gate.astype(BF16)
    rest = w_gate - high.astype(F32)
    mid = rest.astype(BF16)
    low = (rest - mid.astype(F32)).astype(BF16)
    logits = (
        jnp.dot(tokens, low, preferred_element_type=F32)
        + jnp.dot(tokens, mid, preferred_element_type=F32)
        + jnp.dot(tokens, high, preferred_element_type=F32)
    )
    odds = jnp.exp(logits - jnp.max(logits, axis=1, keepdims=True))
    probs = odds / jnp.sum(odds, axis=1, keepdims=True)
    expert = iota((tokens.shape[0], num_experts), 1).astype(F32)
    gate_one = jnp.sum(jnp.where(expert == first, probs, 0.0), axis=1, keepdims=True)
    gate_two = jnp.sum(jnp.where(expert == second, probs, 0.0), axis=1, keepdims=True)
    total = gate_one + gate_two
    return gate_one / total, gate_two / total


def route_kernel(local_experts, capacity, tokens_ref, w_gate_ref, first_ref, second_ref, keep_ref, buffer_ref, plan_ref):
    seq_len = tokens_ref.shape[0]
    num_experts = w_gate_ref.shape[1]
    first, second = first_ref[...], second_ref[...]
    slot_one, slot_two = slots_by_row(first, second, keep_ref[...], num_experts, local_experts, capacity)
    span = buffer_ref.shape[1]
    rows = 256

    @pl.loop(0, local_experts * span // rows)
    def _(step):
        local = step // (span // rows)
        part = step % (span // rows)
        row = iota((rows, seq_len), 0) + step * rows
        pick = jnp.logical_or(row == slot_one, row == slot_two)
        pick = jnp.where(pick, 1.0, 0.0).astype(BF16)
        picked = jnp.dot(pick, tokens_ref[...], preferred_element_type=F32)
        buffer_ref[local, pl.ds(part * rows, rows), :] = picked.astype(BF16)

    columns = columns_of((first, second, slot_one, slot_two), seq_len)
    gate_one, gate_two = gates_of(tokens_ref[...], w_gate_ref[...], columns[:, 0:1], columns[:, 1:2])
    lane = iota((seq_len, 128), 1)
    plan_ref[...] = jnp.where(
        lane == 0, columns[:, 2:3], jnp.where(lane == 1, columns[:, 3:4], jnp.where(lane == 2, gate_one, gate_two))
    )


def exchange_kernel(
    n, local_experts, buffer_ref, w_in_ref, w_out_ref, returned_ref,
    recv, w_in, w_out, hidden, send_sem, recv_sem, back_sem, w_sem,
):
    me = lax.axis_index("ep")
    model_dim, ff_dim = w_in.shape[1:]
    capacity = buffer_ref.shape[2]
    span = n * capacity

    def fetch(e):
        return (
            pltpu.make_async_copy(w_in_ref.at[e], w_in.at[e % 2], w_sem.at[0, e % 2]),
            pltpu.make_async_copy(w_out_ref.at[e], w_out.at[e % 2], w_sem.at[1, e % 2]),
        )

    barrier = pltpu.get_barrier_semaphore()

    @pl.loop(1, n)
    def _(k):
        pl.semaphore_signal(barrier, inc=1, device_id={"ep": lax.rem(me + k, n)}, device_id_type=pl.DeviceIdType.MESH)

    for copy in fetch(0):
        copy.start()
    pl.semaphore_wait(barrier, n - 1)

    def send(source, target, sem, e):
        @pl.loop(1, n)
        def _(k):
            peer = lax.rem(me + k, n)
            pltpu.make_async_remote_copy(
                src_ref=source.at[e, peer],
                dst_ref=target.at[e, me],
                send_sem=send_sem,
                recv_sem=sem.at[e],
                device_id={"ep": peer},
                device_id_type=pl.DeviceIdType.MESH,
            ).start()

    for e in range(local_experts):
        send(buffer_ref, recv, recv_sem, e)
        recv[e, me] = buffer_ref[e, me]

    for e in range(local_experts):
        if e + 1 < local_experts:
            for copy in fetch(e + 1):
                copy.start()
        arrived = recv.at[e, pl.ds(0, n - 1)]
        pltpu.make_async_copy(arrived, arrived, recv_sem.at[e]).wait()
        into, out = fetch(e)
        into.wait()
        wide = 512

        @pl.loop(0, ff_dim // wide)
        def _(j):
            at = pl.ds(pl.multiple_of(j * wide, wide), wide)
            up = jnp.dot(recv[e].reshape(span, model_dim), w_in[e % 2, :, at], preferred_element_type=F32)
            hidden[:, at] = jnp.maximum(up, 0.0).astype(BF16)

        out.wait()
        tall = 256

        @pl.loop(0, span // tall)
        def _(i):
            at = pl.ds(pl.multiple_of(i * tall, tall), tall)
            down = jnp.dot(hidden[at, :], w_out[e % 2], preferred_element_type=F32)
            hidden[at, 0:model_dim] = down.astype(BF16)

        recv[e] = hidden[:, 0:model_dim].reshape(n, capacity, model_dim)
        send(recv, returned_ref, back_sem, e)
        own = pltpu.make_async_copy(recv.at[e, me], returned_ref.at[e, me], w_sem.at[2, 0])
        own.start()
        own.wait()

    for e in range(local_experts):
        arrived = returned_ref.at[e, pl.ds(0, n - 1)]
        pltpu.make_async_copy(arrived, arrived, back_sem.at[e]).wait()
    sent = recv.at[:, pl.ds(0, n - 1)]
    pltpu.make_async_copy(sent, sent, send_sem).wait()
    pltpu.make_async_copy(sent, sent, send_sem).wait()


def combine_kernel(plan_ref, rows_ref, out_ref):
    seq_len = out_ref.shape[0]
    slots = rows_ref.shape[0]
    tall = 256

    @pl.loop(0, seq_len // tall)
    def _(i):
        at = pl.ds(pl.multiple_of(i * tall, tall), tall)
        plan = plan_ref[at, :]
        slot = iota((tall, slots), 1).astype(F32)
        pick = jnp.where(slot == plan[:, 0:1], 1.0, 0.0).astype(BF16)
        total = plan[:, 2:3] * jnp.dot(pick, rows_ref[...], preferred_element_type=F32)
        pick = jnp.where(slot == plan[:, 1:2], 1.0, 0.0).astype(BF16)
        total = total + plan[:, 3:4] * jnp.dot(pick, rows_ref[...], preferred_element_type=F32)
        out_ref[at, :] = total.astype(BF16)


def solution(mesh):
    n = mesh.shape["ep"]
    token_spec = P(("dp", "ep"))
    vmem = pl.BlockSpec(memory_space=pltpu.VMEM)
    hbm = pl.BlockSpec(memory_space=pl.ANY)

    def device_step(tokens, w_gate, first_ids, second_ids, keep_two, w_in, w_out):
        seq_len, model_dim = tokens.shape
        num_experts = w_gate.shape[1]
        local_experts, _, ff_dim = w_in.shape
        capacity = max(2, (2 * seq_len + num_experts - 1) // num_experts)
        span = n * capacity
        buffer, plan = pl.pallas_call(
            functools.partial(route_kernel, local_experts, capacity),
            out_shape=(
                jax.ShapeDtypeStruct((local_experts, span, model_dim), BF16),
                jax.ShapeDtypeStruct((seq_len, 128), F32),
            ),
            in_specs=[vmem] * 5,
            out_specs=(vmem, vmem),
            compiler_params=pltpu.CompilerParams(vmem_limit_bytes=VMEM_LIMIT),
        )(tokens, w_gate, first_ids[None], second_ids[None], keep_two[None])
        slab = (local_experts, n, capacity, model_dim)
        returned = pl.pallas_call(
            functools.partial(exchange_kernel, n, local_experts),
            out_shape=jax.ShapeDtypeStruct(slab, BF16),
            in_specs=[vmem, hbm, hbm],
            out_specs=hbm,
            scratch_shapes=[
                pltpu.VMEM(slab, BF16),
                pltpu.VMEM((2, model_dim, ff_dim), BF16),
                pltpu.VMEM((2, ff_dim, model_dim), BF16),
                pltpu.VMEM((span, ff_dim), BF16),
                pltpu.SemaphoreType.DMA,
                pltpu.SemaphoreType.DMA((local_experts,)),
                pltpu.SemaphoreType.DMA((local_experts,)),
                pltpu.SemaphoreType.DMA((3, 2)),
            ],
            compiler_params=pltpu.CompilerParams(collective_id=0, has_side_effects=True, vmem_limit_bytes=VMEM_LIMIT),
        )(buffer.reshape(slab), w_in, w_out)
        return pl.pallas_call(
            combine_kernel,
            out_shape=jax.ShapeDtypeStruct((seq_len, model_dim), BF16),
            in_specs=[vmem, vmem],
            out_specs=vmem,
            compiler_params=pltpu.CompilerParams(vmem_limit_bytes=VMEM_LIMIT),
        )(plan, returned.reshape(local_experts * span, model_dim))

    return jax.shard_map(
        device_step,
        mesh=mesh,
        in_specs=(P(("dp", "ep"), None), P(), token_spec, token_spec, token_spec, P("ep"), P("ep")),
        out_specs=P(("dp", "ep"), None),
        check_vma=False,
    )
```

```python
import functools
import math
import jax
import jax.numpy as jnp
from jax import lax
from jax.experimental import pallas as pl
from jax.experimental.pallas import tpu as pltpu
from jax.sharding import PartitionSpec as P

F32, BF16, I32 = jnp.float32, jnp.bfloat16, jnp.int32
VMEM_LIMIT = 67_000_000


def iota(shape, axis):
    return lax.broadcasted_iota(I32, shape, axis)


def peer_offsets(n):
    side = math.isqrt(n // 2)
    cells = [(dy, dx) for dy in range(side) for dx in range(side) if dy or dx]
    near = {step: min(step, side - step) for step in range(side)}
    cells.sort(key=lambda cell: (-near[cell[0]] - near[cell[1]], cell))
    order = [(0, 0, 0), (0, 0, 1)] + [(dy, dx, core) for core in range(2) for dy, dx in cells]
    return side, order


def row_of(ref):
    return jnp.concatenate([ref[i : i + 1, :] for i in range(ref.shape[0])], axis=1)


def slots_by_row(first, second, keep, num_experts, local_experts, capacity, place):
    seq_len = first.shape[1]
    block = 256
    expert = iota((num_experts, seq_len), 0)
    hot_first = (expert == first).astype(F32)
    hot_second = (expert == second).astype(F32)
    hot_kept = hot_second * keep.astype(F32)
    hot = jnp.concatenate([hot_first, hot_kept], axis=0)
    before = (iota((block, block), 0) < iota((block, block), 1)).astype(BF16)
    count = jnp.zeros((2 * num_experts, 1), F32)
    earlier = []
    for start in range(0, seq_len, block):
        part = hot[:, start : start + block]
        earlier.append(jnp.dot(part.astype(BF16), before, preferred_element_type=F32) + count)
        count = count + jnp.sum(part, axis=1, keepdims=True)
    earlier = jnp.concatenate(earlier, axis=1)
    pos_one = jnp.sum(earlier[:num_experts] * hot_first, axis=0, keepdims=True)
    pos_two = jnp.sum((earlier[num_experts:] + count[:num_experts]) * hot_second, axis=0, keepdims=True)
    pos_one, pos_two = pos_one.astype(I32), pos_two.astype(I32)
    span = num_experts // local_experts * capacity

    def slot(ids, pos, kept):
        return jnp.where(kept, (ids % local_experts) * span + place(ids // local_experts) * capacity + pos, -1)

    kept_two = jnp.logical_and(pos_two < capacity, keep > 0)
    return slot(first, pos_one, pos_one < capacity), slot(second, pos_two, kept_two)


def columns_of(rows, seq_len):
    sublane = iota((128, seq_len), 0)
    stacked = jnp.zeros((128, seq_len), F32)
    for i, row in enumerate(rows):
        stacked = jnp.where(sublane == i, row.astype(F32), stacked)
    return stacked.T


def gates_of(tokens, w_gate, first, second):
    num_experts = w_gate.shape[1]
    high = w_gate.astype(BF16)
    rest = w_gate - high.astype(F32)
    mid = rest.astype(BF16)
    low = (rest - mid.astype(F32)).astype(BF16)
    logits = (
        jnp.dot(tokens, low, preferred_element_type=F32)
        + jnp.dot(tokens, mid, preferred_element_type=F32)
        + jnp.dot(tokens, high, preferred_element_type=F32)
    )
    odds = jnp.exp(logits - jnp.max(logits, axis=1, keepdims=True))
    probs = odds / jnp.sum(odds, axis=1, keepdims=True)
    expert = iota((tokens.shape[0], num_experts), 1).astype(F32)
    gate_one = jnp.sum(jnp.where(expert == first, probs, 0.0), axis=1, keepdims=True)
    gate_two = jnp.sum(jnp.where(expert == second, probs, 0.0), axis=1, keepdims=True)
    total = gate_one + gate_two
    return gate_one / total, gate_two / total


def layer_kernel(
    n, local_experts, capacity, tokens_hbm, w_gate_ref, first_ref, second_ref, keep_ref, w_in_ref, w_out_ref, out_ref,
    tokens, buffer, recv, returned, w_in, w_out, hidden, total, plan, send_sem, recv_sem, back_sem, w_sem, tok_sem,
):
    me = lax.axis_index("ep")
    seq_len, model_dim = tokens.shape
    num_experts = w_gate_ref.shape[1]
    ff_dim = w_in.shape[2]
    span = n * capacity
    side, order = peer_offsets(n)
    my_core, my_x, my_y = me % 2, me // 2 % side, me // (2 * side)
    group = 8
    rows = group * capacity

    def fetch(e):
        return (
            pltpu.make_async_copy(w_in_ref.at[e], w_in.at[e % 2], w_sem.at[0, e % 2]),
            pltpu.make_async_copy(w_out_ref.at[e], w_out.at[e % 2], w_sem.at[1, e % 2]),
        )

    load = pltpu.make_async_copy(tokens_hbm, tokens, tok_sem)
    load.start()
    barrier = pltpu.get_barrier_semaphore()

    @pl.loop(1, n)
    def _(k):
        pl.semaphore_signal(barrier, inc=1, device_id={"ep": lax.rem(me + k, n)}, device_id_type=pl.DeviceIdType.MESH)

    for e in range(min(2, local_experts)):
        for copy in fetch(e):
            copy.start()

    def place(device):
        core = (device - my_core) % 2
        x = (device // 2 - my_x + side) % side
        y = (device // (2 * side) - my_y + side) % side
        flat = (y * side + x) * 2 + core
        at = jnp.zeros_like(device)
        for i, (dy, dx, dc) in enumerate(order):
            at = jnp.where(flat == (dy * side + dx) * 2 + dc, i, at)
        return at

    first, second, keep = row_of(first_ref), row_of(second_ref), row_of(keep_ref)
    slot_one, slot_two = slots_by_row(first, second, keep, num_experts, local_experts, capacity, place)

    def send(source, target, sem, e, part):
        for i in range(part * group, (part + 1) * group):
            if i == 0:
                continue
            dy, dx, dc = order[i]
            back = order.index(((side - dy) % side, (side - dx) % side, dc))
            peer = ((my_y + dy) % side * side + (my_x + dx) % side) * 2 + (my_core + dc) % 2
            pltpu.make_async_remote_copy(
                src_ref=source.at[e, i],
                dst_ref=target.at[e, back],
                send_sem=send_sem,
                recv_sem=sem.at[e],
                device_id={"ep": peer},
                device_id_type=pl.DeviceIdType.MESH,
            ).start()

    def build(e, part):
        row = iota((rows, seq_len), 0) + (e * span + part * rows)
        pick = jnp.logical_or(row == slot_one, row == slot_two)
        pick = jnp.where(pick, 1.0, 0.0).astype(BF16)
        picked = jnp.dot(pick, tokens[...], preferred_element_type=F32).astype(BF16)
        buffer[e, part * group : (part + 1) * group] = picked.reshape(group, capacity, model_dim)

    parts = n // group
    load.wait()
    pl.semaphore_wait(barrier, n - 1)

    @pl.loop(0, local_experts)
    def _(e):
        for part in range(parts):
            build(e, part)
            if part:
                send(buffer, recv, recv_sem, e, part - 1)
        recv[e, 0] = buffer[e, 0]
        send(buffer, recv, recv_sem, e, parts - 1)

    columns = columns_of((first, second, slot_one, slot_two), seq_len)
    gate_one, gate_two = gates_of(tokens[...], w_gate_ref[...], columns[:, 0:1], columns[:, 1:2])
    lane = iota((seq_len, 128), 1)
    plan[...] = jnp.where(
        lane == 0, columns[:, 2:3], jnp.where(lane == 1, columns[:, 3:4], jnp.where(lane == 2, gate_one, gate_two))
    )

    for e in range(local_experts):
        arrived = recv.at[e, pl.ds(1, n - 1)]
        pltpu.make_async_copy(arrived, arrived, recv_sem.at[e]).wait()
        into, out = fetch(e)
        into.wait()
        wide = 512

        @pl.loop(0, ff_dim // wide)
        def _(j):
            at = pl.ds(pl.multiple_of(j * wide, wide), wide)
            up = jnp.dot(recv[e].reshape(span, model_dim), w_in[e % 2, :, at], preferred_element_type=F32)
            hidden[:, at] = jnp.maximum(up, 0.0).astype(BF16)

        out.wait()
        for part in range(parts):
            down = jnp.dot(hidden[part * rows : (part + 1) * rows, :], w_out[e % 2], preferred_element_type=F32)
            recv[e, part * group : (part + 1) * group] = down.astype(BF16).reshape(group, capacity, model_dim)
            if part:
                send(recv, returned, back_sem, e, part - 1)
        returned[e, 0] = recv[e, 0]
        send(recv, returned, back_sem, e, parts - 1)
        if e + 2 < local_experts:
            for copy in fetch(e + 2):
                copy.start()

    tall = 256
    for e in range(local_experts):
        arrived = returned.at[e, pl.ds(1, n - 1)]
        pltpu.make_async_copy(arrived, arrived, back_sem.at[e]).wait()

        @pl.loop(0, seq_len // tall)
        def _(i):
            at = pl.ds(pl.multiple_of(i * tall, tall), tall)
            part = plan[at, :]
            slot = (iota((tall, span), 1) + e * span).astype(F32)
            pick = jnp.concatenate(
                [jnp.where(slot == part[:, c : c + 1], 1.0, 0.0).astype(BF16) for c in range(2)], axis=0
            )
            picked = jnp.dot(pick, returned[e].reshape(span, model_dim), preferred_element_type=F32)
            added = part[:, 2:3] * picked[:tall] + part[:, 3:4] * picked[tall:]
            if e:
                added = total[at, :] + added
            if e + 1 < local_experts:
                total[at, :] = added
            else:
                out_ref[at, :] = added.astype(BF16)

    sent = recv.at[:, pl.ds(1, n - 1)]
    pltpu.make_async_copy(sent, sent, send_sem).wait()
    pltpu.make_async_copy(sent, sent, send_sem).wait()


def solution(mesh):
    n = mesh.shape["ep"]
    token_spec = P(("dp", "ep"))
    vmem = pl.BlockSpec(memory_space=pltpu.VMEM)
    hbm = pl.BlockSpec(memory_space=pl.ANY)

    def device_step(tokens, w_gate, first_ids, second_ids, keep_two, w_in, w_out):
        seq_len, model_dim = tokens.shape
        num_experts = w_gate.shape[1]
        local_experts, _, ff_dim = w_in.shape
        capacity = max(2, (2 * seq_len + num_experts - 1) // num_experts)
        slab = (local_experts, n, capacity, model_dim)
        lanes = (seq_len // 128, 128)
        return pl.pallas_call(
            functools.partial(layer_kernel, n, local_experts, capacity),
            out_shape=jax.ShapeDtypeStruct((seq_len, model_dim), BF16),
            in_specs=[hbm, vmem, vmem, vmem, vmem, hbm, hbm],
            out_specs=vmem,
            scratch_shapes=[
                pltpu.VMEM((seq_len, model_dim), BF16),
                pltpu.VMEM(slab, BF16),
                pltpu.VMEM(slab, BF16),
                pltpu.VMEM(slab, BF16),
                pltpu.VMEM((2, model_dim, ff_dim), BF16),
                pltpu.VMEM((2, ff_dim, model_dim), BF16),
                pltpu.VMEM((n * capacity, ff_dim), BF16),
                pltpu.VMEM((seq_len, model_dim), F32),
                pltpu.VMEM((seq_len, 128), F32),
                pltpu.SemaphoreType.DMA,
                pltpu.SemaphoreType.DMA((local_experts,)),
                pltpu.SemaphoreType.DMA((local_experts,)),
                pltpu.SemaphoreType.DMA((2, 2)),
                pltpu.SemaphoreType.DMA,
            ],
            compiler_params=pltpu.CompilerParams(collective_id=0, has_side_effects=True, vmem_limit_bytes=VMEM_LIMIT),
        )(
            tokens, w_gate, first_ids.reshape(lanes), second_ids.reshape(lanes), keep_two.reshape(lanes), w_in, w_out
        )

    return jax.shard_map(
        device_step,
        mesh=mesh,
        in_specs=(P(("dp", "ep"), None), P(), token_spec, token_spec, token_spec, P("ep"), P("ep")),
        out_specs=P(("dp", "ep"), None),
        check_vma=False,
    )
```

```python
import functools
import math
import jax
import jax.numpy as jnp
from jax import lax
from jax.experimental import pallas as pl
from jax.experimental.pallas import tpu as pltpu
from jax.sharding import PartitionSpec as P

F32, BF16, I32 = jnp.float32, jnp.bfloat16, jnp.int32
VMEM_LIMIT = 56_000_000


def iota(shape, axis):
    return lax.broadcasted_iota(I32, shape, axis)


def peer_offsets(n):
    side = math.isqrt(n // 2)
    cells = [(dy, dx) for dy in range(side) for dx in range(side) if dy or dx]
    near = {step: min(step, side - step) for step in range(side)}
    cells.sort(key=lambda cell: (-near[cell[0]] - near[cell[1]], cell))
    order = [(0, 0, 0), (0, 0, 1)] + [(*cell, (i + half) % 2) for half in range(2) for i, cell in enumerate(cells)]
    return side, order


def row_of(ref):
    return jnp.concatenate([ref[i : i + 1, :] for i in range(ref.shape[0])], axis=1)


def slots_by_row(first, second, keep, num_experts, local_experts, capacity, place):
    seq_len = first.shape[1]
    block = 256
    expert = iota((num_experts, seq_len), 0)
    hot_first = (expert == first).astype(F32)
    hot_second = (expert == second).astype(F32)
    hot_kept = hot_second * keep.astype(F32)
    hot = jnp.concatenate([hot_first, hot_kept], axis=0)
    before = (iota((block, block), 0) < iota((block, block), 1)).astype(BF16)
    count = jnp.zeros((2 * num_experts, 1), F32)
    earlier = []
    for start in range(0, seq_len, block):
        part = hot[:, start : start + block]
        earlier.append(jnp.dot(part.astype(BF16), before, preferred_element_type=F32) + count)
        count = count + jnp.sum(part, axis=1, keepdims=True)
    earlier = jnp.concatenate(earlier, axis=1)
    pos_one = jnp.sum(earlier[:num_experts] * hot_first, axis=0, keepdims=True)
    pos_two = jnp.sum((earlier[num_experts:] + count[:num_experts]) * hot_second, axis=0, keepdims=True)
    pos_one, pos_two = pos_one.astype(I32), pos_two.astype(I32)
    span = num_experts // local_experts * capacity

    def slot(ids, pos, kept):
        return jnp.where(kept, (ids % local_experts) * span + place(ids // local_experts) * capacity + pos, -1)

    kept_two = jnp.logical_and(pos_two < capacity, keep > 0)
    return slot(first, pos_one, pos_one < capacity), slot(second, pos_two, kept_two)


def columns_of(rows, seq_len):
    sublane = iota((128, seq_len), 0)
    stacked = jnp.zeros((128, seq_len), F32)
    for i, row in enumerate(rows):
        stacked = jnp.where(sublane == i, row.astype(F32), stacked)
    return stacked.T


def gates_of(tokens, w_gate, first, second):
    num_experts = w_gate.shape[1]
    high = w_gate.astype(BF16)
    rest = w_gate - high.astype(F32)
    mid = rest.astype(BF16)
    low = (rest - mid.astype(F32)).astype(BF16)
    logits = (
        jnp.dot(tokens, low, preferred_element_type=F32)
        + jnp.dot(tokens, mid, preferred_element_type=F32)
        + jnp.dot(tokens, high, preferred_element_type=F32)
    )
    odds = jnp.exp(logits - jnp.max(logits, axis=1, keepdims=True))
    probs = odds / jnp.sum(odds, axis=1, keepdims=True)
    expert = iota((tokens.shape[0], num_experts), 1).astype(F32)
    gate_one = jnp.sum(jnp.where(expert == first, probs, 0.0), axis=1, keepdims=True)
    gate_two = jnp.sum(jnp.where(expert == second, probs, 0.0), axis=1, keepdims=True)
    total = gate_one + gate_two
    return gate_one / total, gate_two / total


def layer_kernel(
    n, local_experts, capacity, tokens_hbm, w_gate_ref, first_ref, second_ref, keep_ref, w_in_ref, w_out_ref, out_ref,
    tokens, buffer, recv, returned, w_in, w_out, hidden, total, plan, send_sem, recv_sem, back_sem, w_sem, tok_sem,
):
    me = lax.axis_index("ep")
    seq_len, model_dim = tokens.shape
    num_experts = w_gate_ref.shape[1]
    ff_dim = w_in.shape[2]
    span = n * capacity
    side, order = peer_offsets(n)
    my_core, my_x, my_y = me % 2, me // 2 % side, me // (2 * side)
    group = 8
    rows = group * capacity

    def fetch(e):
        return (
            pltpu.make_async_copy(w_in_ref.at[e], w_in.at[e % 2], w_sem.at[0, e % 2]),
            pltpu.make_async_copy(w_out_ref.at[e], w_out.at[e % 2], w_sem.at[1, e % 2]),
        )

    load = pltpu.make_async_copy(tokens_hbm, tokens, tok_sem)
    load.start()
    barrier = pltpu.get_barrier_semaphore()

    @pl.loop(1, n)
    def _(k):
        pl.semaphore_signal(barrier, inc=1, device_id={"ep": lax.rem(me + k, n)}, device_id_type=pl.DeviceIdType.MESH)

    for e in range(min(2, local_experts)):
        for copy in fetch(e):
            copy.start()

    def place(device):
        core = (device - my_core) % 2
        x = (device // 2 - my_x + side) % side
        y = (device // (2 * side) - my_y + side) % side
        flat = (y * side + x) * 2 + core
        at = jnp.zeros_like(device)
        for i, (dy, dx, dc) in enumerate(order):
            at = jnp.where(flat == (dy * side + dx) * 2 + dc, i, at)
        return at

    first, second, keep = row_of(first_ref), row_of(second_ref), row_of(keep_ref)
    slot_one, slot_two = slots_by_row(first, second, keep, num_experts, local_experts, capacity, place)

    def by_core(zero, one):
        return zero + my_core * (one - zero)

    def send(source, target, sem, e, part):
        for at in range(max(part * group, 1), (part + 1) * group):
            slots = (at, n - at)
            dy, dx, dc = (by_core(*pair) for pair in zip(*(order[i] for i in slots)))
            back = by_core(*(order.index((-order[i][0] % side, -order[i][1] % side, order[i][2])) for i in slots))
            peer = ((my_y + dy) % side * side + (my_x + dx) % side) * 2 + (my_core + dc) % 2
            pltpu.make_async_remote_copy(
                src_ref=source.at[e, by_core(*slots)],
                dst_ref=target.at[e, back],
                send_sem=send_sem,
                recv_sem=sem.at[e],
                device_id={"ep": peer},
                device_id_type=pl.DeviceIdType.MESH,
            ).start()

    def wait(ref, sem, e):
        arrived = ref.at[e, pl.ds(1, n - 1)]
        pltpu.make_async_copy(arrived, arrived, sem.at[e]).wait()

    parts = n // group
    load.wait()

    @pl.loop(0, local_experts * parts)
    def _(step):
        e, part = step // parts, step % parts
        built = by_core(part, parts - 1 - part)
        row = iota((rows, seq_len), 0) + (e * span + built * rows)
        pick = jnp.logical_or(row == slot_one, row == slot_two)
        pick = jnp.where(pick, 1.0, 0.0).astype(BF16)
        picked = jnp.dot(pick, tokens[...], preferred_element_type=F32).astype(BF16)
        buffer[e, pl.ds(built * group, group)] = picked.reshape(group, capacity, model_dim)

        @pl.when(step == 0)
        def _():
            pl.semaphore_wait(barrier, n - 1)

        for last in range(parts):
            @pl.when(jnp.logical_and(step > 0, part == (last + 1) % parts))
            def _():
                send(buffer, recv, recv_sem, (step - 1) // parts, last)

    total[...] = jnp.zeros_like(total)
    for e in range(local_experts):
        recv[e, 0] = buffer[e, 0]
    send(buffer, recv, recv_sem, local_experts - 1, parts - 1)

    columns = columns_of((first, second, slot_one, slot_two), seq_len)
    gate_one, gate_two = gates_of(tokens[...], w_gate_ref[...], columns[:, 0:1], columns[:, 1:2])
    lane = iota((seq_len, 128), 1)
    plan[...] = jnp.where(
        lane == 0, columns[:, 2:3], jnp.where(lane == 1, columns[:, 3:4], jnp.where(lane == 2, gate_one, gate_two))
    )

    @pl.loop(0, local_experts)
    def _(e):
        wait(recv, recv_sem, e)
        into, out = fetch(e)
        into.wait()
        wide = 512

        @pl.loop(0, ff_dim // wide)
        def _(j):
            at = pl.ds(pl.multiple_of(j * wide, wide), wide)
            up = jnp.dot(recv[e].reshape(span, model_dim), w_in[e % 2, :, at], preferred_element_type=F32)
            hidden[:, at] = jnp.maximum(up, 0.0).astype(BF16)

        out.wait()

        @pl.loop(0, parts)
        def _(part):
            built = by_core(part, parts - 1 - part)
            at = pl.ds(pl.multiple_of(built * rows, rows), rows)
            down = jnp.dot(hidden[at, :], w_out[e % 2], preferred_element_type=F32)
            recv[e, pl.ds(built * group, group)] = down.astype(BF16).reshape(group, capacity, model_dim)
            for last in range(parts - 1):
                @pl.when(part == last + 1)
                def _():
                    send(recv, returned, back_sem, e, last)

        returned[e, 0] = recv[e, 0]
        send(recv, returned, back_sem, e, parts - 1)

        @pl.when(e + 2 < local_experts)
        def _():
            for copy in fetch(e + 2):
                copy.start()

    tall = 256

    def combine(e, final):
        wait(returned, back_sem, e)

        @pl.loop(0, seq_len // tall)
        def _(i):
            at = pl.ds(pl.multiple_of(i * tall, tall), tall)
            part = plan[at, :]
            slot = (iota((tall, span), 1) + e * span).astype(F32)
            pick = jnp.concatenate(
                [jnp.where(slot == part[:, c : c + 1], 1.0, 0.0).astype(BF16) for c in range(2)], axis=0
            )
            picked = jnp.dot(pick, returned[e].reshape(span, model_dim), preferred_element_type=F32)
            added = total[at, :] + (part[:, 2:3] * picked[:tall] + part[:, 3:4] * picked[tall:])
            if final:
                out_ref[at, :] = added.astype(BF16)
            else:
                total[at, :] = added

    @pl.loop(0, local_experts - 1)
    def _(e):
        combine(e, False)

    combine(local_experts - 1, True)

    sent = recv.at[:, pl.ds(1, n - 1)]
    pltpu.make_async_copy(sent, sent, send_sem).wait()
    pltpu.make_async_copy(sent, sent, send_sem).wait()


def solution(mesh):
    n = mesh.shape["ep"]
    token_spec = P(("dp", "ep"))
    vmem = pl.BlockSpec(memory_space=pltpu.VMEM)
    hbm = pl.BlockSpec(memory_space=pl.ANY)

    def device_step(tokens, w_gate, first_ids, second_ids, keep_two, w_in, w_out):
        seq_len, model_dim = tokens.shape
        num_experts = w_gate.shape[1]
        local_experts, _, ff_dim = w_in.shape
        capacity = max(2, (2 * seq_len + num_experts - 1) // num_experts)
        slab = (local_experts, n, capacity, model_dim)
        lanes = (seq_len // 128, 128)
        return pl.pallas_call(
            functools.partial(layer_kernel, n, local_experts, capacity),
            out_shape=pltpu.VMEM((seq_len, model_dim), BF16),
            in_specs=[hbm, vmem, vmem, vmem, vmem, hbm, hbm],
            out_specs=vmem,
            scratch_shapes=[
                pltpu.VMEM((seq_len, model_dim), BF16),
                pltpu.VMEM(slab, BF16),
                pltpu.VMEM(slab, BF16),
                pltpu.VMEM(slab, BF16),
                pltpu.VMEM((2, model_dim, ff_dim), BF16),
                pltpu.VMEM((2, ff_dim, model_dim), BF16),
                pltpu.VMEM((n * capacity, ff_dim), BF16),
                pltpu.VMEM((seq_len, model_dim), F32),
                pltpu.VMEM((seq_len, 128), F32),
                pltpu.SemaphoreType.DMA,
                pltpu.SemaphoreType.DMA((local_experts,)),
                pltpu.SemaphoreType.DMA((local_experts,)),
                pltpu.SemaphoreType.DMA((2, 2)),
                pltpu.SemaphoreType.DMA,
            ],
            compiler_params=pltpu.CompilerParams(collective_id=0, has_side_effects=True, vmem_limit_bytes=VMEM_LIMIT),
        )(
            tokens, w_gate, first_ids.reshape(lanes), second_ids.reshape(lanes), keep_two.reshape(lanes), w_in, w_out
        )

    return jax.shard_map(
        device_step,
        mesh=mesh,
        in_specs=(P(("dp", "ep"), None), P(), token_spec, token_spec, token_spec, P("ep"), P("ep")),
        out_specs=P(("dp", "ep"), None),
        check_vma=False,
    )
```
